32 devices in a mesh: gx: 4 (over y, x), gy: 2 (over core), ha: 4 (over z).
Axes of the slice: x: 2, y: 2, z: 4, core: 2. Of those that a mesh axis runs over, the one named last changes fastest.
Arguments:
- level_set: float32 [32, 32, 40, 128], P('gx', 'gy', 'ha'), may hold values from -4 to 4
- wind_field: float32 [2, 32, 32], P(None, 'gx', 'gy'), may hold values from -3 to 3
Outputs:
- increment: float32 [32, 32, 40, 128], P('gx', 'gy', 'ha')
The draws below stay inside these ranges and needn't reach their ends.
All inputs are finite; a program needn't handle non-finite values.
Results may differ from the reference program's by a relative error of at most 0.000073.
Values sent between devices are 32-bit elements; how exact they have to be, the bound alone decides.
A program may use at most 128 MiB of HBM per device.

```python
import math
import jax
import jax.numpy as jnp
from jax import lax

NV = 128
NX = 32
NY = 32
NH = 40


CELL_SIZE = 0.05


def draw_level_set(key, part):
    rough_key = jax.random.fold_in(key, 11)
    center_key = jax.random.fold_in(key, 12)
    shape = (NX, NY, NH, NV)
    centers = jax.random.uniform(center_key, (2,), jnp.float32, 0.3, 0.7)
    pos_x = (jnp.arange(NX, dtype=jnp.float32) + 0.5) / NX
    pos_y = (jnp.arange(NY, dtype=jnp.float32) + 0.5) / NY
    span_x = (pos_x - centers[0]) * NX * CELL_SIZE
    span_y = (pos_y - centers[1]) * NY * CELL_SIZE
    smooth = jnp.sqrt(span_x[:, None] ** 2 + span_y[None, :] ** 2 + 0.01) - 0.25 * NX * CELL_SIZE
    smooth = smooth[:, :, None, None]
    rough = 0.5 * jax.random.normal(rough_key, shape, jnp.float32)
    surface = rough + smooth
    return jnp.clip(surface, -4.0, 4.0)


def draw_wind_field(key, part):
    raw_key = jax.random.fold_in(key, 21)
    shape = (2, NX, NY)
    ramp = 0.1 + 2.9 * (jnp.arange(NX, dtype=jnp.float32) + 0.5) / NX
    raw = jax.random.uniform(raw_key, shape, jnp.float32, -1.0, 1.0)
    return raw * ramp[None, :, None]


def setup_inputs(seed: int = 0) -> dict:
    streams_of = jax.random.split(jax.random.key(seed), 3)
    return {
        "level_set": draw_level_set(jax.random.fold_in(streams_of[2], 71), 0),
        "wind_field": draw_wind_field(jax.random.fold_in(streams_of[2], 71), 0),
    }


CELL_SIZE = 0.05
SPEED_LOW = 0.1
SPEED_SPAN = 0.4
TURN_MAX = 1.0
ACCEL_MAX = 0.05
CFL_NUMBER = 0.5
WENO_EPS = 1e-6


def ghost_rows(values, along, at_low):
    length = values.shape[along]
    if at_low:
        edge_row = lax.slice_in_dim(values, 0, 1, axis=along)
        next_row = lax.slice_in_dim(values, 1, 2, axis=along)
        reaches = (3.0, 2.0, 1.0)
    else:
        edge_row = lax.slice_in_dim(values, length - 1, length, axis=along)
        next_row = lax.slice_in_dim(values, length - 2, length - 1, axis=along)
        reaches = (1.0, 2.0, 3.0)
    slope_edge = edge_row - next_row
    return jnp.concatenate([edge_row + distance * slope_edge for distance in reaches], axis=along)


def extend(values, along):
    return jnp.concatenate([ghost_rows(values, along, True), values, ghost_rows(values, along, False)], axis=along)


def speed_shifts(values):
    length = values.shape[3]
    below_rows = ghost_rows(values, 3, True)
    above_rows = ghost_rows(values, 3, False)
    shifted = []
    for displace in range(-3, 4):
        pieces = []
        if displace < 0:
            pieces.append(lax.slice_in_dim(below_rows, 3 + displace, 3, axis=3))
        pieces.append(lax.slice_in_dim(values, max(displace, 0), length + min(displace, 0), axis=3))
        if displace > 0:
            pieces.append(lax.slice_in_dim(above_rows, 0, displace, axis=3))
        shifted.append(jnp.concatenate(pieces, axis=3) if len(pieces) > 1 else pieces[0])
    return shifted


def weno_side(left_far, left_near, middle, right_near, right_far):
    guess_one = left_far * (1.0 / 3.0) - left_near * (7.0 / 6.0) + middle * (11.0 / 6.0)
    guess_two = -left_near * (1.0 / 6.0) + middle * (5.0 / 6.0) + right_near * (1.0 / 3.0)
    guess_three = middle * (1.0 / 3.0) + right_near * (5.0 / 6.0) - right_far * (1.0 / 6.0)
    smooth_one = (13.0 / 12.0) * jnp.square(left_far - 2.0 * left_near + middle) + 0.25 * jnp.square(left_far - 4.0 * left_near + 3.0 * middle)
    smooth_two = (13.0 / 12.0) * jnp.square(left_near - 2.0 * middle + right_near) + 0.25 * jnp.square(left_near - right_near)
    smooth_three = (13.0 / 12.0) * jnp.square(middle - 2.0 * right_near + right_far) + 0.25 * jnp.square(3.0 * middle - 4.0 * right_near + right_far)
    weight_one = 0.1 / jnp.square(smooth_one + WENO_EPS)
    weight_two = 0.6 / jnp.square(smooth_two + WENO_EPS)
    weight_three = 0.3 / jnp.square(smooth_three + WENO_EPS)
    return (weight_one * guess_one + weight_two * guess_two + weight_three * guess_three) / (weight_one + weight_two + weight_three)


def weno_pair(shifted, spacing):
    slopes = [(shifted[position + 1] - shifted[position]) / spacing for position in range(6)]
    left_slope = weno_side(slopes[0], slopes[1], slopes[2], slopes[3], slopes[4])
    right_slope = weno_side(slopes[5], slopes[4], slopes[3], slopes[2], slopes[1])
    return left_slope, right_slope


def cell_rates(cos_head, sin_head, speeds, wind_x, wind_y, d_theta, d_speed):
    along_x = speeds[None, None, None, :] * cos_head[None, None, :, None] + wind_x[:, :, None, None]
    along_y = speeds[None, None, None, :] * sin_head[None, None, :, None] + wind_y[:, :, None, None]
    return jnp.abs(along_x) / CELL_SIZE + jnp.abs(along_y) / CELL_SIZE + TURN_MAX / d_theta + ACCEL_MAX / d_speed


def hamilton(x_pair, y_pair, head_pair, speed_pair, cos_head, sin_head, speeds, wind_x, wind_y):
    flow_x = speeds[None, None, None, :] * cos_head[None, None, :, None] + wind_x[:, :, None, None]
    flow_y = speeds[None, None, None, :] * sin_head[None, None, :, None] + wind_y[:, :, None, None]
    mean_x = 0.5 * (x_pair[0] + x_pair[1])
    mean_y = 0.5 * (y_pair[0] + y_pair[1])
    mean_head = 0.5 * (head_pair[0] + head_pair[1])
    mean_speed = 0.5 * (speed_pair[0] + speed_pair[1])
    value = -(flow_x * mean_x + flow_y * mean_y + TURN_MAX * jnp.abs(mean_head) + ACCEL_MAX * jnp.abs(mean_speed))
    damping = 0.5 * (jnp.abs(flow_x) * (x_pair[1] - x_pair[0]) + jnp.abs(flow_y) * (y_pair[1] - y_pair[0])
                     + TURN_MAX * (head_pair[1] - head_pair[0]) + ACCEL_MAX * (speed_pair[1] - speed_pair[0]))
    return -jnp.maximum(value - damping, 0.0)


def reference(level_set, wind_field):
    d_theta = 2.0 * math.pi / NH
    d_speed = SPEED_SPAN / NV
    angles = jnp.arange(NH, dtype=jnp.int32).astype(jnp.float32) * d_theta
    cos_head = jnp.cos(angles)
    sin_head = jnp.sin(angles)
    speeds = SPEED_LOW + SPEED_SPAN * (jnp.arange(NV, dtype=jnp.int32).astype(jnp.float32) + 0.5) / NV
    rows_all = jnp.arange(NX, dtype=jnp.int32)

    def plane_max(position):
        winds = lax.dynamic_slice_in_dim(wind_field, position, 1, 1)
        return jnp.max(cell_rates(cos_head, sin_head, speeds, winds[0], winds[1], d_theta, d_speed))

    time_step = CFL_NUMBER / jnp.max(lax.map(plane_max, rows_all))

    def advance(surface):
        x_padded = extend(surface, 0)

        def one_plane(position):
            x_plane = lax.dynamic_slice_in_dim(surface, position, 1, 0)
            x_shifted = [lax.dynamic_slice_in_dim(x_padded, position + 3 + displace, 1, 0) for displace in range(-3, 4)]
            y_padded = extend(x_plane, 1)
            y_shifted = [y_padded[:, 3 + displace:3 + displace + NY] for displace in range(-3, 4)]
            head_padded = jnp.concatenate([x_plane[:, :, NH - 3:], x_plane, x_plane[:, :, :3]], axis=2)
            head_shifted = [head_padded[:, :, 3 + displace:3 + displace + NH] for displace in range(-3, 4)]
            winds = lax.dynamic_slice_in_dim(wind_field, position, 1, 1)
            return hamilton(weno_pair(x_shifted, CELL_SIZE), weno_pair(y_shifted, CELL_SIZE),
                            weno_pair(head_shifted, d_theta), weno_pair(speed_shifts(x_plane), d_speed),
                            cos_head, sin_head, speeds, winds[0], winds[1])

        return lax.map(one_plane, rows_all).reshape(surface.shape)

    section_one = level_set + time_step * advance(level_set)
    section_two = 0.75 * level_set + 0.25 * (section_one + time_step * advance(section_one))
    advanced = (1.0 / 3.0) * level_set + (2.0 / 3.0) * (section_two + time_step * advance(section_two))
    return advanced - level_set
```

```python
import functools
import math

import jax
import jax.numpy as jnp
import numpy as np
from jax import lax
from jax.experimental import pallas as pl
from jax.experimental.pallas import tpu as pltpu
from jax.sharding import PartitionSpec as P

CELL_SIZE = 0.05
SPEED_LOW = 0.1
SPEED_SPAN = 0.4
TURN_MAX = 1.0
ACCEL_MAX = 0.05
CFL_NUMBER = 0.5
WENO_EPS = 1e-06
SCALE = 32.0
PAD = 8
MESH = pl.DeviceIdType.MESH


def rcp(d):
    x = pl.reciprocal(d, approx=True)
    return x * (2.0 - d * x)


def eps_of(spacing):
    return 0.75 * WENO_EPS * (spacing * SCALE) ** 2


def upwind(dm2, dm1, d0, dp1, dp2, c0, c1, fh, eps):
    pos = fh > 0.0
    d1 = jnp.where(pos, dp2, dm2)
    d2 = jnp.where(pos, dp1, dm1)
    d4 = jnp.where(pos, dm1, dp1)
    c = jnp.where(pos, c1, c0)
    d3 = d0
    e1 = d2 - d1
    e2 = d3 - d2
    e3 = d4 - d3
    g2 = 0.75 * d2
    g3 = 0.75 * d3
    s1 = e1 * e1 + (g2 * (d2 + e1) + eps)
    s2 = e2 * e2 + (g2 * d3 + eps)
    s3 = e3 * e3 + (g3 * (d3 - e3) + eps)
    t1 = s2 * s3
    t2 = s1 * s3
    t3 = s1 * s2
    r1 = t1 * t1
    r2 = t2 * t2
    w3 = 1.5 * (t3 * t3)
    num = r1 * (e1 - e2) + w3 * (e2 - e3)
    den = (r1 + 6.0 * r2) + (w3 + w3)
    q = (d3 + 0.5 * d2) + num * rcp(den)
    return q * (jnp.abs(fh) * (1.0 / 3.0)) - c * fh


def triple(da, db, eps):
    e = db - da
    s2 = e * e + (0.75 * (da * db) + eps)
    h = 1.5 * e
    return e, s2 + db * h, s2, s2 - da * h


def face_pair(c, d2, d3, e1, e2, e3, s1, s2, s3):
    t1 = s2 * s3
    t2 = s1 * s3
    t3 = s1 * s2
    r1 = t1 * t1
    r2 = t2 * t2
    r3 = t3 * t3
    a = r1 * (e1 - e2)
    b = r3 * (e2 - e3)
    m = 6.0 * r2 + (r1 + r3)
    n = a + b
    left = (3.0 * c + (d3 + 0.5 * d2)) + (n + 0.5 * b) * rcp(m + (r3 + r3))
    right = ((d2 + 0.5 * d3) - 3.0 * c) + (n + 0.5 * a) * rcp(m + (r1 + r1))
    return left, right


def kernel(sizes, axes, u_ref, wind_ref, flow_ref, rate_ref, out_ref,
           b0, b1, b2, acc, wind, best, peers, step, sends, recvs, rsend, rrecv):
    nx, ny, nh, nv = sizes
    ngx, ngy, nha = axes
    bufs = (b0, b1, b2)
    d_theta = 2.0 * math.pi / (nh * nha)
    d_speed = SPEED_SPAN / nv
    tiles = ny // 8
    gx, gy, ha = lax.axis_index("gx"), lax.axis_index("gy"), lax.axis_index("ha")
    n_xy = ngx * ngy
    me = gx * ngy + gy

    def peer(delta):
        other = lax.rem(me + delta, n_xy)
        return {"gx": other // ngy, "gy": lax.rem(other, ngy)}

    up_ha = {"ha": lax.rem(ha + 1, nha)}
    down_ha = {"ha": lax.rem(ha + nha - 1, nha)}
    barrier = pltpu.get_barrier_semaphore()
    for delta in range(1, n_xy):
        pl.semaphore_signal(barrier, inc=1, device_id=peer(delta), device_id_type=MESH)
    for target in (up_ha, down_ha):
        pl.semaphore_signal(barrier, inc=1, device_id=target, device_id_type=MESH)

    def load_plane(x, carry):
        for k in range(nh):
            b0[3 + x, 3 + k, PAD:PAD + ny, :] = u_ref[x, k] * SCALE
        for comp in range(2):
            for y in range(ny):
                wind[comp, x, y:y + 1, :] = jnp.full((1, nv), wind_ref[comp, x, y], jnp.float32)
        return carry

    lax.fori_loop(0, nx, load_plane, 0)

    def rate_plane(x, top):
        for r in range(rate_ref.shape[1]):
            for t in range(tiles):
                fx = rate_ref[0, r:r + 1, :] + wind[0, x, 8 * t:8 * t + 8, :]
                fy = rate_ref[1, r:r + 1, :] + wind[1, x, 8 * t:8 * t + 8, :]
                top = jnp.maximum(top, (jnp.abs(fx) + jnp.abs(fy)) * (1.0 / CELL_SIZE))
        return top

    best[...] = lax.fori_loop(0, nx, rate_plane, jnp.zeros((8, 128), jnp.float32))

    pl.semaphore_wait(barrier, n_xy + 1)

    xs, hs, ys = pl.ds(3, nx), pl.ds(3, nh), pl.ds(PAD, ny)

    def copies(s):
        buf = bufs[s]
        plans = (
            (buf.at[pl.ds(nx, 3), hs, ys], buf.at[pl.ds(0, 3), hs, ys], {"gx": gx + 1},
             gx < ngx - 1, gx > 0),
            (buf.at[pl.ds(3, 3), hs, ys], buf.at[pl.ds(3 + nx, 3), hs, ys], {"gx": gx - 1},
             gx > 0, gx < ngx - 1),
            (buf.at[xs, pl.ds(nh, 3), ys], buf.at[xs, pl.ds(0, 3), ys], up_ha, None, None),
            (buf.at[xs, pl.ds(3, 3), ys], buf.at[xs, pl.ds(3 + nh, 3), ys], down_ha, None, None),
            (buf.at[xs, hs, pl.ds(ny, PAD)], buf.at[xs, hs, pl.ds(0, PAD)], {"gy": gy + 1},
             gy < ngy - 1, gy > 0),
            (buf.at[xs, hs, pl.ds(PAD, PAD)], buf.at[xs, hs, pl.ds(PAD + ny, PAD)], {"gy": gy - 1},
             gy > 0, gy < ngy - 1),
        )
        return [
            (pltpu.make_async_remote_copy(
                src_ref=src, dst_ref=dst, send_sem=sends.at[s, i], recv_sem=recvs.at[s, i],
                device_id=target, device_id_type=MESH), has_out, has_in)
            for i, (src, dst, target, has_out, has_in) in enumerate(plans)
        ]

    def under(condition, act):
        if condition is None:
            act()
        else:
            pl.when(condition)(act)

    rate_copies = [
        pltpu.make_async_remote_copy(
            src_ref=best, dst_ref=peers.at[delta - 1], send_sem=rsend.at[delta - 1],
            recv_sem=rrecv.at[delta - 1], device_id=peer(delta), device_id_type=MESH)
        for delta in range(1, n_xy)
    ]
    plans = [copies(s) for s in range(3)]

    def send_all(s):
        for copy, has_out, _ in plans[s]:
            under(has_out, copy.start)

    def wait_in(s, which):
        for i in which:
            copy, _, has_in = plans[s][i]
            under(has_in, copy.wait_recv)

    def v_pass(buf):
        eps = eps_of(d_speed)
        coef = ACCEL_MAX / (3.0 * d_speed)
        e4 = np.float32(np.float32(eps * eps) ** 2)
        edge = lax.broadcasted_iota(jnp.int32, (ny, nv), 1) == 0

        def one(u):
            up = lambda a: pltpu.roll(a, 1, 1)
            down = lambda a: pltpu.roll(a, nv - 1, 1)
            q = u - up(u)
            q = jnp.where(edge, down(q), q)
            qm = up(q)
            d = jnp.where(edge, 0.0, q - qm)
            d3 = down(d)
            e2, f1, s2, f3 = triple(d, d3, eps)
            e1, e3, s1, s3 = up(e2), down(e2), up(f1), down(f3)
            t1 = s2 * s3
            t2 = s1 * s3
            t3 = s1 * s2
            r1 = t1 * t1
            r2 = t2 * t2
            r3 = t3 * t3
            f12 = e1 - e2
            f23 = e2 - e3
            r2l = jnp.where(edge, r1, r2)
            r3l = jnp.where(edge, e4, r3)
            r2r = jnp.where(edge, r3, r2)
            r1r = jnp.where(edge, e4, r1)
            al = r1 * jnp.where(edge, 0.0, f12)
            bl = r3l * f23
            ar = r1r * f12
            br = r3 * jnp.where(edge, 0.0, f23)
            cr = jnp.where(edge, qm, q)
            left = (3.0 * q + (d3 + 0.5 * d)) + (al + 1.5 * bl) * rcp(r1 + 6.0 * r2l + 3.0 * r3l)
            right = ((d + 0.5 * d3) - 3.0 * cr) + (1.5 * ar + br) * rcp(3.0 * r1r + 6.0 * r2r + r3)
            return coef * jnp.minimum(left, down(right))

        def body(x, carry):
            def inner(k, carry):
                for j in range(2):
                    acc[x, 2 * k + j] = one(buf[3 + x, 3 + 2 * k + j, PAD:PAD + ny, :])
                return carry
            return lax.fori_loop(0, nh // 2, inner, carry)

        lax.fori_loop(0, nx, body, 0)

    def h_pass(buf):
        eps = eps_of(d_theta)
        coef = TURN_MAX / (3.0 * d_theta)

        def body(i, carry):
            x = i // tiles
            rows = pl.ds(pl.multiple_of(lax.rem(i, tiles) * 8, 8) + PAD, 8)
            rows_acc = pl.ds(pl.multiple_of(lax.rem(i, tiles) * 8, 8), 8)
            u = [buf[3 + x, j, rows, :] for j in range(nh + 6)]
            q = [u[j + 1] - u[j] for j in range(nh + 5)]
            d = [q[j + 1] - q[j] for j in range(nh + 4)]
            tr = [triple(d[j], d[j + 1], eps) for j in range(nh + 3)]
            before = None
            for f in range(nh + 1):
                left, right = face_pair(
                    q[f + 2], d[f + 1], d[f + 2], tr[f][0], tr[f + 1][0], tr[f + 2][0],
                    tr[f][1], tr[f + 1][2], tr[f + 2][3])
                if before is not None:
                    acc[x, f - 1, rows_acc, :] += coef * jnp.minimum(before, right)
                before = left
            return carry

        lax.fori_loop(0, nx * tiles, body, 0)

    def flow_row(comp, k):
        return flow_ref[comp, pl.ds(ha * nh + k, 1), :]

    def y_pass(buf):
        eps = eps_of(CELL_SIZE)

        def body(x, carry):
            def inner(k, carry):
                row = flow_row(1, k)
                for t in range(tiles):
                    u = [buf[3 + x, 3 + k, PAD + 8 * t + j:PAD + 8 * t + j + 8, :] for j in range(-3, 4)]
                    q = [u[j + 1] - u[j] for j in range(6)]
                    d = [q[j + 1] - q[j] for j in range(5)]
                    fh = (row + wind[1, x, 8 * t:8 * t + 8, :]) * (1.0 / CELL_SIZE)
                    acc[x, k, 8 * t:8 * t + 8, :] += upwind(*d, q[2], q[3], fh, eps)
                return carry
            return lax.fori_loop(0, nh, inner, carry)

        lax.fori_loop(0, nx, body, 0)

    def x_pass(s):
        buf = bufs[s]
        eps = eps_of(CELL_SIZE)

        def body(i, carry):
            k = i // tiles
            base = pl.multiple_of(lax.rem(i, tiles) * 8, 8)
            rows, rows_acc = pl.ds(base + PAD, 8), pl.ds(base, 8)
            row = flow_row(0, k)
            dt = step[...]
            u = [buf[j, 3 + k, rows, :] for j in range(nx + 6)]
            q = [u[j + 1] - u[j] for j in range(nx + 5)]
            d = [q[j + 1] - q[j] for j in range(nx + 4)]
            for x in range(nx):
                fh = (row + wind[0, x, rows_acc, :]) * (1.0 / CELL_SIZE)
                total = acc[x, k, rows_acc, :] + upwind(*d[x:x + 5], q[x + 2], q[x + 3], fh, eps)
                moved = u[x + 3] - dt * jnp.maximum(total, 0.0)
                if s == 0:
                    b1[3 + x, 3 + k, rows, :] = moved
                elif s == 1:
                    b2[3 + x, 3 + k, rows, :] = 0.75 * b0[3 + x, 3 + k, rows, :] + 0.25 * moved
                else:
                    out_ref[x, k, rows_acc, :] = (moved - b0[3 + x, 3 + k, rows, :]) * (2.0 / (3.0 * SCALE))
            return carry

        lax.fori_loop(0, nh * tiles, body, 0)

    def fill_x(buf):
        def ends(low):
            def act():
                def body(k, carry):
                    edge = buf[3 if low else nx + 2, 3 + k, PAD:PAD + ny, :]
                    slope = edge - buf[4 if low else nx + 1, 3 + k, PAD:PAD + ny, :]
                    for r in range(1, 4):
                        buf[3 - r if low else nx + 2 + r, 3 + k, PAD:PAD + ny, :] = edge + r * slope
                    return carry
                lax.fori_loop(0, nh, body, 0)
            return act
        pl.when(gx == 0)(ends(True))
        pl.when(gx == ngx - 1)(ends(False))

    def fill_y(buf):
        index = lax.broadcasted_iota(jnp.int32, (8, nv), 0).astype(jnp.float32)

        def ends(low):
            reach = (8.0 - index) if low else (index + 1.0)
            at, near, to = (PAD, PAD + 1, 0) if low else (PAD + ny - 1, PAD + ny - 2, PAD + ny)

            def act():
                def body(x, carry):
                    def inner(k, carry):
                        edge = buf[3 + x, 3 + k, at:at + 1, :]
                        slope = edge - buf[3 + x, 3 + k, near:near + 1, :]
                        buf[3 + x, 3 + k, to:to + 8, :] = edge + reach * slope
                        return carry
                    return lax.fori_loop(0, nh, inner, carry)
                lax.fori_loop(0, nx, body, 0)
            return act
        pl.when(gy == 0)(ends(True))
        pl.when(gy == ngy - 1)(ends(False))

    for s in range(3):
        send_all(s)
        if s == 0:
            for copy in rate_copies:
                copy.start()
        v_pass(bufs[s])
        fill_y(bufs[s])
        fill_x(bufs[s])
        wait_in(s, (4, 5))
        y_pass(bufs[s])
        wait_in(s, (2, 3))
        h_pass(bufs[s])
        if s == 0:
            for copy in rate_copies:
                copy.wait_recv()
            top = best[...]
            for delta in range(1, n_xy):
                top = jnp.maximum(top, peers[delta - 1])
            rate = jnp.max(top, axis=(0, 1), keepdims=True) + (TURN_MAX / d_theta + ACCEL_MAX / d_speed)
            step[...] = jnp.broadcast_to(CFL_NUMBER / rate, step.shape)
        wait_in(s, (0, 1))
        x_pass(s)

    for copy in rate_copies:
        copy.wait_send()
    for s in range(3):
        for copy, has_out, _ in plans[s]:
            under(has_out, copy.wait_send)


def tables(nv, n_head):
    speeds = (SPEED_LOW + SPEED_SPAN * (np.arange(nv, dtype=np.float32) + np.float32(0.5)) / nv).astype(np.float32)
    angles = np.arange(n_head, dtype=np.float32) * np.float32(2.0 * math.pi / n_head)
    turns = np.stack([np.cos(angles.astype(np.float64)), np.sin(angles.astype(np.float64))]).astype(np.float32)
    flow = turns[:, :, None] * speeds[None, None, :]
    ends = np.concatenate([flow[:, :, 0], flow[:, :, -1]], axis=1)
    rows = -(-ends.shape[1] // 128)
    ends = np.concatenate([ends, np.repeat(ends[:, :1], rows * 128 - ends.shape[1], axis=1)], axis=1)
    return flow, ends.reshape(2, rows, 128)


def solution(mesh):
    axes = (mesh.shape["gx"], mesh.shape["gy"], mesh.shape["ha"])

    def body(level_set, wind_field):
        nx, ny, nh, nv = level_set.shape
        flow, ends = tables(nv, nh * axes[2])
        n_xy = axes[0] * axes[1]
        state = pltpu.VMEM((nx + 6, nh + 6, ny + 2 * PAD, nv), jnp.float32)
        vmem = pl.BlockSpec(memory_space=pltpu.VMEM)
        increment = pl.pallas_call(
            functools.partial(kernel, (nx, ny, nh, nv), axes),
            out_shape=jax.ShapeDtypeStruct((nx, nh, ny, nv), jnp.float32),
            in_specs=[vmem, pl.BlockSpec(memory_space=pltpu.SMEM), vmem, vmem],
            out_specs=vmem,
            scratch_shapes=[
                state, state, state,
                pltpu.VMEM((nx, nh, ny, nv), jnp.float32),
                pltpu.VMEM((2, nx, ny, nv), jnp.float32),
                pltpu.VMEM((8, 128), jnp.float32),
                pltpu.VMEM((n_xy - 1, 8, 128), jnp.float32),
                pltpu.VMEM((8, nv), jnp.float32),
                pltpu.SemaphoreType.DMA((3, 6)),
                pltpu.SemaphoreType.DMA((3, 6)),
                pltpu.SemaphoreType.DMA((n_xy - 1,)),
                pltpu.SemaphoreType.DMA((n_xy - 1,)),
            ],
            compiler_params=pltpu.CompilerParams(
                collective_id=0, has_side_effects=True, vmem_limit_bytes=56 * 2**20
            ),
        )(level_set.transpose(0, 2, 1, 3), wind_field, jnp.asarray(flow), jnp.asarray(ends))
        return increment.transpose(0, 2, 1, 3)

    return jax.shard_map(
        body,
        mesh=mesh,
        in_specs=(P("gx", "gy", "ha", None), P(None, "gx", "gy")),
        out_specs=P("gx", "gy", "ha", None),
        check_vma=False,
    )
```

```python
import functools
import math

import jax
import jax.numpy as jnp
import numpy as np
from jax import lax
from jax.experimental import pallas as pl
from jax.experimental.pallas import tpu as pltpu
from jax.sharding import PartitionSpec as P

CELL_SIZE = 0.05
SPEED_LOW = 0.1
SPEED_SPAN = 0.4
TURN_MAX = 1.0
ACCEL_MAX = 0.05
CFL_NUMBER = 0.5
WENO_EPS = 1e-06
SCALE = 32.0
PAD = 8
MESH = pl.DeviceIdType.MESH


def rcp(d):
    x = pl.reciprocal(d, approx=True)
    return x * (2.0 - d * x)


def eps_of(spacing):
    return 0.75 * WENO_EPS * (spacing * SCALE) ** 2


def upwind(dm2, dm1, d0, dp1, dp2, c0, c1, fh, eps):
    pos = fh > 0.0
    d1 = jnp.where(pos, dp2, dm2)
    d2 = jnp.where(pos, dp1, dm1)
    d4 = jnp.where(pos, dm1, dp1)
    c = jnp.where(pos, c1, c0)
    d3 = d0
    e1 = d2 - d1
    e2 = d3 - d2
    e3 = d4 - d3
    g2 = 0.75 * d2
    g3 = 0.75 * d3
    s1 = e1 * e1 + (g2 * (d2 + e1) + eps)
    s2 = e2 * e2 + (g2 * d3 + eps)
    s3 = e3 * e3 + (g3 * (d3 - e3) + eps)
    t1 = s2 * s3
    t2 = s1 * s3
    t3 = s1 * s2
    r1 = t1 * t1
    r2 = t2 * t2
    w3 = 1.5 * (t3 * t3)
    num = r1 * (e1 - e2) + w3 * (e2 - e3)
    den = (r1 + 6.0 * r2) + (w3 + w3)
    q = (d3 + 0.5 * d2) + num * rcp(den)
    return q * (jnp.abs(fh) * (1.0 / 3.0)) - c * fh


def triple(da, db, eps):
    e = db - da
    s2 = e * e + (0.75 * (da * db) + eps)
    h = 1.5 * e
    return e, s2 + db * h, s2, s2 - da * h


def face_pair(c, d2, d3, e1, e2, e3, s1, s2, s3):
    t1 = s2 * s3
    t2 = s1 * s3
    t3 = s1 * s2
    r1 = t1 * t1
    r2 = t2 * t2
    r3 = t3 * t3
    a = r1 * (e1 - e2)
    b = r3 * (e2 - e3)
    m = 6.0 * r2 + (r1 + r3)
    n = a + b
    left = (3.0 * c + (d3 + 0.5 * d2)) + (n + 0.5 * b) * rcp(m + (r3 + r3))
    right = ((d2 + 0.5 * d3) - 3.0 * c) + (n + 0.5 * a) * rcp(m + (r1 + r1))
    return left, right


def kernel(sizes, axes, u_ref, wind_ref, flow_ref, rate_ref, out_ref,
           b0, b1, b2, acc, shifted, rights, wind, best, peers, step, sends, recvs, rsend, rrecv):
    nx, ny, nh, nv = sizes
    ngx, ngy, nha = axes
    bufs = (b0, b1, b2)
    d_theta = 2.0 * math.pi / (nh * nha)
    d_speed = SPEED_SPAN / nv
    tiles = ny // 8
    gx, gy, ha = lax.axis_index("gx"), lax.axis_index("gy"), lax.axis_index("ha")
    n_xy = ngx * ngy
    me = gx * ngy + gy

    def peer(delta):
        other = lax.rem(me + delta, n_xy)
        return {"gx": other // ngy, "gy": lax.rem(other, ngy)}

    up_ha = {"ha": lax.rem(ha + 1, nha)}
    down_ha = {"ha": lax.rem(ha + nha - 1, nha)}
    barrier = pltpu.get_barrier_semaphore()
    for delta in range(1, n_xy):
        pl.semaphore_signal(barrier, inc=1, device_id=peer(delta), device_id_type=MESH)
    for target in (up_ha, down_ha):
        pl.semaphore_signal(barrier, inc=1, device_id=target, device_id_type=MESH)

    def load_plane(x, carry):
        for k in range(nh):
            b0[3 + x, 3 + k, PAD:PAD + ny, :] = u_ref[x, k] * SCALE
        for comp in range(2):
            for y in range(ny):
                wind[comp, x, y:y + 1, :] = jnp.full((1, nv), wind_ref[comp, x, y], jnp.float32)
        return carry

    lax.fori_loop(0, nx, load_plane, 0)

    def rate_plane(x, top):
        for r in range(rate_ref.shape[1]):
            for t in range(tiles):
                fx = rate_ref[0, r:r + 1, :] + wind[0, x, 8 * t:8 * t + 8, :]
                fy = rate_ref[1, r:r + 1, :] + wind[1, x, 8 * t:8 * t + 8, :]
                top = jnp.maximum(top, (jnp.abs(fx) + jnp.abs(fy)) * (1.0 / CELL_SIZE))
        return top

    best[...] = lax.fori_loop(0, nx, rate_plane, jnp.zeros((8, 128), jnp.float32))

    pl.semaphore_wait(barrier, n_xy + 1)

    xs, hs, ys = pl.ds(3, nx), pl.ds(3, nh), pl.ds(PAD, ny)

    def copies(s):
        buf = bufs[s]
        plans = (
            (buf.at[pl.ds(nx, 3), hs, ys], buf.at[pl.ds(0, 3), hs, ys], {"gx": gx + 1},
             gx < ngx - 1, gx > 0),
            (buf.at[pl.ds(3, 3), hs, ys], buf.at[pl.ds(3 + nx, 3), hs, ys], {"gx": gx - 1},
             gx > 0, gx < ngx - 1),
            (buf.at[xs, pl.ds(nh, 3), ys], buf.at[xs, pl.ds(0, 3), ys], up_ha, None, None),
            (buf.at[xs, pl.ds(3, 3), ys], buf.at[xs, pl.ds(3 + nh, 3), ys], down_ha, None, None),
            (buf.at[xs, hs, pl.ds(ny, PAD)], buf.at[xs, hs, pl.ds(0, PAD)], {"gy": gy + 1},
             gy < ngy - 1, gy > 0),
            (buf.at[xs, hs, pl.ds(PAD, PAD)], buf.at[xs, hs, pl.ds(PAD + ny, PAD)], {"gy": gy - 1},
             gy > 0, gy < ngy - 1),
        )
        return [
            (pltpu.make_async_remote_copy(
                src_ref=src, dst_ref=dst, send_sem=sends.at[s, i], recv_sem=recvs.at[s, i],
                device_id=target, device_id_type=MESH), has_out, has_in)
            for i, (src, dst, target, has_out, has_in) in enumerate(plans)
        ]

    def under(condition, act):
        if condition is None:
            act()
        else:
            pl.when(condition)(act)

    rate_copies = [
        pltpu.make_async_remote_copy(
            src_ref=best, dst_ref=peers.at[delta - 1], send_sem=rsend.at[delta - 1],
            recv_sem=rrecv.at[delta - 1], device_id=peer(delta), device_id_type=MESH)
        for delta in range(1, n_xy)
    ]
    plans = [copies(s) for s in range(3)]

    def send_all(s):
        for copy, has_out, _ in plans[s]:
            under(has_out, copy.start)

    def wait_in(s, which):
        for i in which:
            copy, _, has_in = plans[s][i]
            under(has_in, copy.wait_recv)

    def v_shift(buf):
        def body(i, carry):
            for j in range(2):
                for k in range(nh):
                    u = buf[3 + 2 * i + j, 3 + k, PAD:PAD + ny, :]
                    for at, move in enumerate((3, 2, 1, nv - 1, nv - 2)):
                        shifted[at, 2 * i + j, k] = pltpu.roll(u, move, 1)
            return carry

        lax.fori_loop(0, nx // 2, body, 0)

    def v_pass(buf):
        eps = eps_of(d_speed)
        coef = ACCEL_MAX / (3.0 * d_speed)
        e4 = np.float32(np.float32(eps * eps) ** 2)
        lane = lax.broadcasted_iota(jnp.int32, (8, nv), 1)
        edge = lane == 0
        keep1 = jnp.where((lane == 1) | (lane == 2), 0.0, 1.0)
        keep2 = jnp.where(lane < 2, 0.0, 1.0)
        keep3 = jnp.where((lane == 0) | (lane == nv - 1), 0.0, 1.0)
        keep4 = jnp.where(lane >= nv - 2, 0.0, 1.0)
        inner_lane = jnp.where(edge, 0.0, 1.0)

        def one(x, k, t):
            rows = slice(8 * t, 8 * t + 8)
            u0 = buf[3 + x, 3 + k, PAD + 8 * t:PAD + 8 * t + 8, :]
            um3, um2, um1, up1, up2 = [shifted[at, x, k, rows, :] for at in range(5)]
            qa, qb, qc, qd, qe = um2 - um3, um1 - um2, u0 - um1, up1 - u0, up2 - up1
            d1 = (qb - qa) * keep1
            d2 = (qc - qb) * keep2
            d3 = (qd - qc) * keep3
            d4 = (qe - qd) * keep4
            e1 = d2 - d1
            e2 = d3 - d2
            e3 = d4 - d3
            g2 = 0.75 * d2
            g3 = 0.75 * d3
            s1 = e1 * e1 + (g2 * (d2 + e1) + eps)
            s2 = e2 * e2 + (g2 * d3 + eps)
            s3 = e3 * e3 + (g3 * (d3 - e3) + eps)
            t1 = s2 * s3
            t2 = s1 * s3
            t3 = s1 * s2
            r1 = t1 * t1
            r2 = t2 * t2
            r3 = t3 * t3
            f12 = e1 - e2
            f23 = e2 - e3
            r2l = jnp.where(edge, r1, r2)
            r3l = jnp.where(edge, e4, r3)
            r2r = jnp.where(edge, r3, r2)
            r1r = jnp.where(edge, e4, r1)
            cl = jnp.where(edge, qd, qc)
            cr = jnp.where(edge, qb, qc)
            nl = r1 * (f12 * inner_lane) + 1.5 * (r3l * f23)
            nr = 1.5 * (r1r * f12) + r3 * (f23 * inner_lane)
            left = (3.0 * cl + (d3 + 0.5 * d2)) + nl * rcp(r1 + 6.0 * r2l + 3.0 * r3l)
            right = ((d2 + 0.5 * d3) - 3.0 * cr) + nr * rcp(3.0 * r1r + 6.0 * r2r + r3)
            acc[x, k, rows, :] = coef * left
            rights[x, k, rows, :] = coef * right

        def body(x, carry):
            def inner(k, carry):
                for j in range(2):
                    for t in range(tiles):
                        one(x, 2 * k + j, t)
                return carry
            return lax.fori_loop(0, nh // 2, inner, carry)

        lax.fori_loop(0, nx, body, 0)

    def h_pass(buf):
        eps = eps_of(d_theta)
        coef = TURN_MAX / (3.0 * d_theta)

        def body(i, carry):
            x = i // tiles
            rows = pl.ds(pl.multiple_of(lax.rem(i, tiles) * 8, 8) + PAD, 8)
            rows_acc = pl.ds(pl.multiple_of(lax.rem(i, tiles) * 8, 8), 8)
            u = [buf[3 + x, j, rows, :] for j in range(nh + 6)]
            q = [u[j + 1] - u[j] for j in range(nh + 5)]
            d = [q[j + 1] - q[j] for j in range(nh + 4)]
            tr = [triple(d[j], d[j + 1], eps) for j in range(nh + 3)]
            before = None
            for f in range(nh + 1):
                left, right = face_pair(
                    q[f + 2], d[f + 1], d[f + 2], tr[f][0], tr[f + 1][0], tr[f + 2][0],
                    tr[f][1], tr[f + 1][2], tr[f + 2][3])
                if before is not None:
                    acc[x, f - 1, rows_acc, :] += coef * jnp.minimum(before, right)
                before = left
            return carry

        lax.fori_loop(0, nx * tiles, body, 0)

    def flow_row(comp, k):
        return flow_ref[comp, pl.ds(ha * nh + k, 1), :]

    def y_pass(buf):
        eps = eps_of(CELL_SIZE)

        group = math.gcd(nh, 5)

        def one(x, k, row, t):
            u = [buf[3 + x, 3 + k, PAD + 8 * t + j:PAD + 8 * t + j + 8, :] for j in range(-3, 4)]
            q = [u[j + 1] - u[j] for j in range(6)]
            d = [q[j + 1] - q[j] for j in range(5)]
            fh = (row + wind[1, x, 8 * t:8 * t + 8, :]) * (1.0 / CELL_SIZE)
            return upwind(*d, q[2], q[3], fh, eps)

        def body(x, carry):
            def inner(g, carry):
                speed = [pltpu.roll(rights[x, group * g + j], nv - 1, 1) for j in range(group)]
                for j in range(group):
                    k = group * g + j
                    row = flow_row(1, k)
                    for t in range(tiles):
                        rows = slice(8 * t, 8 * t + 8)
                        along_v = jnp.minimum(acc[x, k, rows, :], speed[j][rows])
                        acc[x, k, rows, :] = along_v + one(x, k, row, t)
                return carry
            return lax.fori_loop(0, nh // group, inner, carry)

        lax.fori_loop(0, nx, body, 0)

    def x_pass(s):
        buf = bufs[s]
        eps = eps_of(CELL_SIZE)

        def body(i, carry):
            k = i // tiles
            base = pl.multiple_of(lax.rem(i, tiles) * 8, 8)
            rows, rows_acc = pl.ds(base + PAD, 8), pl.ds(base, 8)
            row = flow_row(0, k)
            dt = step[...]
            u = [buf[j, 3 + k, rows, :] for j in range(nx + 6)]
            q = [u[j + 1] - u[j] for j in range(nx + 5)]
            d = [q[j + 1] - q[j] for j in range(nx + 4)]
            for x in range(nx):
                fh = (row + wind[0, x, rows_acc, :]) * (1.0 / CELL_SIZE)
                total = acc[x, k, rows_acc, :] + upwind(*d[x:x + 5], q[x + 2], q[x + 3], fh, eps)
                moved = u[x + 3] - dt * jnp.maximum(total, 0.0)
                if s == 0:
                    b1[3 + x, 3 + k, rows, :] = moved
                elif s == 1:
                    b2[3 + x, 3 + k, rows, :] = 0.75 * b0[3 + x, 3 + k, rows, :] + 0.25 * moved
                else:
                    out_ref[x, k, rows_acc, :] = (moved - b0[3 + x, 3 + k, rows, :]) * (2.0 / (3.0 * SCALE))
            return carry

        lax.fori_loop(0, nh * tiles, body, 0)

    def fill_x(buf):
        def ends(low):
            def act():
                def body(k, carry):
                    edge = buf[3 if low else nx + 2, 3 + k, PAD:PAD + ny, :]
                    slope = edge - buf[4 if low else nx + 1, 3 + k, PAD:PAD + ny, :]
                    for r in range(1, 4):
                        buf[3 - r if low else nx + 2 + r, 3 + k, PAD:PAD + ny, :] = edge + r * slope
                    return carry
                lax.fori_loop(0, nh, body, 0)
            return act
        pl.when(gx == 0)(ends(True))
        pl.when(gx == ngx - 1)(ends(False))

    def fill_y(buf):
        index = lax.broadcasted_iota(jnp.int32, (8, nv), 0).astype(jnp.float32)

        def ends(low):
            reach = (8.0 - index) if low else (index + 1.0)
            at, near, to = (PAD, PAD + 1, 0) if low else (PAD + ny - 1, PAD + ny - 2, PAD + ny)

            def act():
                def body(x, carry):
                    for k in range(nh):
                        edge = buf[3 + x, 3 + k, at:at + 1, :]
                        slope = edge - buf[3 + x, 3 + k, near:near + 1, :]
                        buf[3 + x, 3 + k, to:to + 8, :] = edge + reach * slope
                    return carry
                lax.fori_loop(0, nx, body, 0)
            return act
        pl.when(gy == 0)(ends(True))
        pl.when(gy == ngy - 1)(ends(False))

    for s in range(3):
        send_all(s)
        if s == 0:
            for copy in rate_copies:
                copy.start()
        v_shift(bufs[s])
        v_pass(bufs[s])
        fill_y(bufs[s])
        fill_x(bufs[s])
        wait_in(s, (4, 5))
        y_pass(bufs[s])
        wait_in(s, (2, 3))
        h_pass(bufs[s])
        if s == 0:
            for copy in rate_copies:
                copy.wait_recv()
            top = best[...]
            for delta in range(1, n_xy):
                top = jnp.maximum(top, peers[delta - 1])
            rate = jnp.max(top, axis=(0, 1), keepdims=True) + (TURN_MAX / d_theta + ACCEL_MAX / d_speed)
            step[...] = jnp.broadcast_to(CFL_NUMBER / rate, step.shape)
        wait_in(s, (0, 1))
        x_pass(s)

    for copy in rate_copies:
        copy.wait_send()
    for s in range(3):
        for copy, has_out, _ in plans[s]:
            under(has_out, copy.wait_send)


def tables(nv, n_head):
    speeds = (SPEED_LOW + SPEED_SPAN * (np.arange(nv, dtype=np.float32) + np.float32(0.5)) / nv).astype(np.float32)
    angles = np.arange(n_head, dtype=np.float32) * np.float32(2.0 * math.pi / n_head)
    turns = np.stack([np.cos(angles.astype(np.float64)), np.sin(angles.astype(np.float64))]).astype(np.float32)
    flow = turns[:, :, None] * speeds[None, None, :]
    ends = np.concatenate([flow[:, :, 0], flow[:, :, -1]], axis=1)
    rows = -(-ends.shape[1] // 128)
    ends = np.concatenate([ends, np.repeat(ends[:, :1], rows * 128 - ends.shape[1], axis=1)], axis=1)
    return flow, ends.reshape(2, rows, 128)


def solution(mesh):
    axes = (mesh.shape["gx"], mesh.shape["gy"], mesh.shape["ha"])

    def body(level_set, wind_field):
        nx, ny, nh, nv = level_set.shape
        flow, ends = tables(nv, nh * axes[2])
        n_xy = axes[0] * axes[1]
        state = pltpu.VMEM((nx + 6, nh + 6, ny + 2 * PAD, nv), jnp.float32)
        vmem = pl.BlockSpec(memory_space=pltpu.VMEM)
        increment = pl.pallas_call(
            functools.partial(kernel, (nx, ny, nh, nv), axes),
            out_shape=jax.ShapeDtypeStruct((nx, nh, ny, nv), jnp.float32),
            in_specs=[vmem, pl.BlockSpec(memory_space=pltpu.SMEM), vmem, vmem],
            out_specs=vmem,
            scratch_shapes=[
                state, state, state,
                pltpu.VMEM((nx, nh, ny, nv), jnp.float32),
                pltpu.VMEM((5, nx, nh, ny, nv), jnp.float32),
                pltpu.VMEM((nx, nh, ny, nv), jnp.float32),
                pltpu.VMEM((2, nx, ny, nv), jnp.float32),
                pltpu.VMEM((8, 128), jnp.float32),
                pltpu.VMEM((n_xy - 1, 8, 128), jnp.float32),
                pltpu.VMEM((8, nv), jnp.float32),
                pltpu.SemaphoreType.DMA((3, 6)),
                pltpu.SemaphoreType.DMA((3, 6)),
                pltpu.SemaphoreType.DMA((n_xy - 1,)),
                pltpu.SemaphoreType.DMA((n_xy - 1,)),
            ],
            compiler_params=pltpu.CompilerParams(
                collective_id=0, has_side_effects=True, vmem_limit_bytes=56 * 2**20
            ),
        )(level_set.transpose(0, 2, 1, 3), wind_field, jnp.asarray(flow), jnp.asarray(ends))
        return increment.transpose(0, 2, 1, 3)

    return jax.shard_map(
        body,
        mesh=mesh,
        in_specs=(P("gx", "gy", "ha", None), P(None, "gx", "gy")),
        out_specs=P("gx", "gy", "ha", None),
        check_vma=False,
    )
```

```python
import functools
import math

import jax
import jax.numpy as jnp
import numpy as np
from jax import lax
from jax.experimental import pallas as pl
from jax.experimental.pallas import tpu as pltpu
from jax.sharding import PartitionSpec as P

CELL_SIZE = 0.05
SPEED_LOW = 0.1
SPEED_SPAN = 0.4
TURN_MAX = 1.0
ACCEL_MAX = 0.05
CFL_NUMBER = 0.5
WENO_EPS = 1e-06
SCALE = 32.0
PAD = 8
MESH = pl.DeviceIdType.MESH


def rcp(d):
    x = pl.reciprocal(d, approx=True)
    return x * (2.0 - d * x)


def eps_of(spacing):
    return 0.75 * WENO_EPS * (spacing * SCALE) ** 2


def upwind(dm2, dm1, d0, dp1, dp2, c0, c1, fh, eps):
    pos = fh > 0.0
    d1 = jnp.where(pos, dp2, dm2)
    d2 = jnp.where(pos, dp1, dm1)
    d4 = jnp.where(pos, dm1, dp1)
    c = jnp.where(pos, c1, c0)
    d3 = d0
    e1 = d2 - d1
    e2 = d3 - d2
    e3 = d4 - d3
    g2 = 0.75 * d2
    g3 = 0.75 * d3
    s1 = e1 * e1 + (g2 * (d2 + e1) + eps)
    s2 = e2 * e2 + (g2 * d3 + eps)
    s3 = e3 * e3 + (g3 * (d3 - e3) + eps)
    t1 = s2 * s3
    t2 = s1 * s3
    t3 = s1 * s2
    r1 = t1 * t1
    r2 = t2 * t2
    w3 = 1.5 * (t3 * t3)
    num = r1 * (e1 - e2) + w3 * (e2 - e3)
    den = (r1 + 6.0 * r2) + (w3 + w3)
    q = (d3 + 0.5 * d2) + num * rcp(den)
    return q * (jnp.abs(fh) * (1.0 / 3.0)) - c * fh


def triple(da, db, eps):
    e = db - da
    s2 = e * e + (0.75 * (da * db) + eps)
    h = 1.5 * e
    return e, s2 + db * h, s2, s2 - da * h


def face_pair(c, d2, d3, e1, e2, e3, s1, s2, s3):
    t1 = s2 * s3
    t2 = s1 * s3
    t3 = s1 * s2
    r1 = t1 * t1
    r2 = t2 * t2
    r3 = t3 * t3
    a = r1 * (e1 - e2)
    b = r3 * (e2 - e3)
    m = 6.0 * r2 + (r1 + r3)
    n = a + b
    left = (3.0 * c + (d3 + 0.5 * d2)) + (n + 0.5 * b) * rcp(m + (r3 + r3))
    right = ((d2 + 0.5 * d3) - 3.0 * c) + (n + 0.5 * a) * rcp(m + (r1 + r1))
    return left, right


def kernel(sizes, axes, u_ref, wind_ref, flow_ref, rate_ref, out_ref,
           b0, b1, b2, acc, shifted, rights, wind, best, peers, step, sends, recvs, rsend, rrecv):
    nx, ny, nh, nv = sizes
    ngx, ngy, nha = axes
    bufs = (b0, b1, b2)
    d_theta = 2.0 * math.pi / (nh * nha)
    d_speed = SPEED_SPAN / nv
    tiles = ny // 8
    gx, gy, ha = lax.axis_index("gx"), lax.axis_index("gy"), lax.axis_index("ha")
    n_xy = ngx * ngy
    me = gx * ngy + gy

    def peer(delta):
        other = lax.rem(me + delta, n_xy)
        return {"gx": other // ngy, "gy": lax.rem(other, ngy)}

    up_ha = {"ha": lax.rem(ha + 1, nha)}
    down_ha = {"ha": lax.rem(ha + nha - 1, nha)}
    barrier = pltpu.get_barrier_semaphore()
    for delta in range(1, n_xy):
        pl.semaphore_signal(barrier, inc=1, device_id=peer(delta), device_id_type=MESH)
    for target in (up_ha, down_ha):
        pl.semaphore_signal(barrier, inc=1, device_id=target, device_id_type=MESH)

    def load_plane(x, carry):
        for k in range(nh):
            b0[3 + x, 3 + k, PAD:PAD + ny, :] = u_ref[x, k] * SCALE
        for comp in range(2):
            for y in range(ny):
                wind[comp, x, y:y + 1, :] = jnp.full((1, nv), wind_ref[comp, x, y], jnp.float32)
        return carry

    lax.fori_loop(0, nx, load_plane, 0)

    def rate_plane(x, top):
        for r in range(rate_ref.shape[1]):
            for t in range(tiles):
                fx = rate_ref[0, r:r + 1, :] + wind[0, x, 8 * t:8 * t + 8, :]
                fy = rate_ref[1, r:r + 1, :] + wind[1, x, 8 * t:8 * t + 8, :]
                top = jnp.maximum(top, (jnp.abs(fx) + jnp.abs(fy)) * (1.0 / CELL_SIZE))
        return top

    best[...] = lax.fori_loop(0, nx, rate_plane, jnp.zeros((8, 128), jnp.float32))

    pl.semaphore_wait(barrier, n_xy + 1)

    xs, hs, ys = pl.ds(3, nx), pl.ds(3, nh), pl.ds(PAD, ny)

    parts = math.gcd(nh, 5)
    part = nh // parts

    def copies(s):
        buf = bufs[s]
        plans = (
            (buf.at[xs, pl.ds(nh, 3), ys], buf.at[xs, pl.ds(0, 3), ys], up_ha, None, None),
            (buf.at[xs, pl.ds(3, 3), ys], buf.at[xs, pl.ds(3 + nh, 3), ys], down_ha, None, None),
            (buf.at[xs, hs, pl.ds(ny, PAD)], buf.at[xs, hs, pl.ds(0, PAD)], {"gy": gy + 1},
             gy < ngy - 1, gy > 0),
            (buf.at[xs, hs, pl.ds(PAD, PAD)], buf.at[xs, hs, pl.ds(PAD + ny, PAD)], {"gy": gy - 1},
             gy > 0, gy < ngy - 1),
        )
        for c in range(parts):
            hc = pl.ds(3 + c * part, part)
            plans += (
                (buf.at[pl.ds(nx, 3), hc, ys], buf.at[pl.ds(0, 3), hc, ys], {"gx": gx + 1},
                 gx < ngx - 1, gx > 0),
                (buf.at[pl.ds(3, 3), hc, ys], buf.at[pl.ds(3 + nx, 3), hc, ys], {"gx": gx - 1},
                 gx > 0, gx < ngx - 1),
            )
        return [
            (pltpu.make_async_remote_copy(
                src_ref=src, dst_ref=dst, send_sem=sends.at[s, i], recv_sem=recvs.at[s, i],
                device_id=target, device_id_type=MESH), has_out, has_in)
            for i, (src, dst, target, has_out, has_in) in enumerate(plans)
        ]

    def under(condition, act):
        if condition is None:
            act()
        else:
            pl.when(condition)(act)

    rate_copies = [
        pltpu.make_async_remote_copy(
            src_ref=best, dst_ref=peers.at[delta - 1], send_sem=rsend.at[delta - 1],
            recv_sem=rrecv.at[delta - 1], device_id=peer(delta), device_id_type=MESH)
        for delta in range(1, n_xy)
    ]
    plans = [copies(s) for s in range(3)]

    def send(s, which):
        for i in which:
            copy, has_out, _ = plans[s][i]
            under(has_out, copy.start)

    def wait_in(s, which):
        for i in which:
            copy, _, has_in = plans[s][i]
            under(has_in, copy.wait_recv)

    def v_shift(buf):
        def body(i, carry):
            for j in range(2):
                for k in range(nh):
                    u = buf[3 + 2 * i + j, 3 + k, PAD:PAD + ny, :]
                    for at, move in enumerate((3, 2, 1, nv - 1, nv - 2)):
                        shifted[at, 2 * i + j, k] = pltpu.roll(u, move, 1)
            return carry

        lax.fori_loop(0, nx // 2, body, 0)

    def v_pass(buf):
        eps = eps_of(d_speed)
        coef = ACCEL_MAX / (3.0 * d_speed)
        e4 = np.float32(np.float32(eps * eps) ** 2)
        lane = lax.broadcasted_iota(jnp.int32, (8, nv), 1)
        edge = lane == 0
        keep1 = jnp.where((lane == 1) | (lane == 2), 0.0, 1.0)
        keep2 = jnp.where(lane < 2, 0.0, 1.0)
        keep3 = jnp.where((lane == 0) | (lane == nv - 1), 0.0, 1.0)
        keep4 = jnp.where(lane >= nv - 2, 0.0, 1.0)
        inner_lane = jnp.where(edge, 0.0, 1.0)

        def one(x, k, t):
            rows = slice(8 * t, 8 * t + 8)
            u0 = buf[3 + x, 3 + k, PAD + 8 * t:PAD + 8 * t + 8, :]
            um3, um2, um1, up1, up2 = [shifted[at, x, k, rows, :] for at in range(5)]
            qa, qb, qc, qd, qe = um2 - um3, um1 - um2, u0 - um1, up1 - u0, up2 - up1
            d1 = (qb - qa) * keep1
            d2 = (qc - qb) * keep2
            d3 = (qd - qc) * keep3
            d4 = (qe - qd) * keep4
            e1 = d2 - d1
            e2 = d3 - d2
            e3 = d4 - d3
            g2 = 0.75 * d2
            g3 = 0.75 * d3
            s1 = e1 * e1 + (g2 * (d2 + e1) + eps)
            s2 = e2 * e2 + (g2 * d3 + eps)
            s3 = e3 * e3 + (g3 * (d3 - e3) + eps)
            t1 = s2 * s3
            t2 = s1 * s3
            t3 = s1 * s2
            r1 = t1 * t1
            r2 = t2 * t2
            r3 = t3 * t3
            f12 = e1 - e2
            f23 = e2 - e3
            r2l = jnp.where(edge, r1, r2)
            r3l = jnp.where(edge, e4, r3)
            r2r = jnp.where(edge, r3, r2)
            r1r = jnp.where(edge, e4, r1)
            cl = jnp.where(edge, qd, qc)
            cr = jnp.where(edge, qb, qc)
            nl = r1 * (f12 * inner_lane) + 1.5 * (r3l * f23)
            nr = 1.5 * (r1r * f12) + r3 * (f23 * inner_lane)
            left = (3.0 * cl + (d3 + 0.5 * d2)) + nl * rcp(r1 + 6.0 * r2l + 3.0 * r3l)
            right = ((d2 + 0.5 * d3) - 3.0 * cr) + nr * rcp(3.0 * r1r + 6.0 * r2r + r3)
            acc[x, k, rows, :] = coef * left
            rights[x, k, rows, :] = coef * right

        def body(x, carry):
            def inner(k, carry):
                for j in range(2):
                    for t in range(tiles):
                        one(x, 2 * k + j, t)
                return carry
            return lax.fori_loop(0, nh // 2, inner, carry)

        lax.fori_loop(0, nx, body, 0)

    def h_pass(buf):
        eps = eps_of(d_theta)
        coef = TURN_MAX / (3.0 * d_theta)

        def body(i, carry):
            x = i // tiles
            rows = pl.ds(pl.multiple_of(lax.rem(i, tiles) * 8, 8) + PAD, 8)
            rows_acc = pl.ds(pl.multiple_of(lax.rem(i, tiles) * 8, 8), 8)
            u = [buf[3 + x, j, rows, :] for j in range(nh + 6)]
            q = [u[j + 1] - u[j] for j in range(nh + 5)]
            d = [q[j + 1] - q[j] for j in range(nh + 4)]
            tr = [triple(d[j], d[j + 1], eps) for j in range(nh + 3)]
            before = None
            for f in range(nh + 1):
                left, right = face_pair(
                    q[f + 2], d[f + 1], d[f + 2], tr[f][0], tr[f + 1][0], tr[f + 2][0],
                    tr[f][1], tr[f + 1][2], tr[f + 2][3])
                if before is not None:
                    acc[x, f - 1, rows_acc, :] += coef * jnp.minimum(before, right)
                before = left
            return carry

        lax.fori_loop(0, nx * tiles, body, 0)

    def flow_row(comp, k):
        return flow_ref[comp, pl.ds(ha * nh + k, 1), :]

    def y_pass(buf):
        eps = eps_of(CELL_SIZE)

        group = math.gcd(nh, 5)

        def one(x, k, row, t):
            u = [buf[3 + x, 3 + k, PAD + 8 * t + j:PAD + 8 * t + j + 8, :] for j in range(-3, 4)]
            q = [u[j + 1] - u[j] for j in range(6)]
            d = [q[j + 1] - q[j] for j in range(5)]
            fh = (row + wind[1, x, 8 * t:8 * t + 8, :]) * (1.0 / CELL_SIZE)
            return upwind(*d, q[2], q[3], fh, eps)

        def body(x, carry):
            def inner(g, carry):
                speed = [pltpu.roll(rights[x, group * g + j], nv - 1, 1) for j in range(group)]
                for j in range(group):
                    k = group * g + j
                    row = flow_row(1, k)
                    for t in range(tiles):
                        rows = slice(8 * t, 8 * t + 8)
                        along_v = jnp.minimum(acc[x, k, rows, :], speed[j][rows])
                        acc[x, k, rows, :] = along_v + one(x, k, row, t)
                return carry
            return lax.fori_loop(0, nh // group, inner, carry)

        lax.fori_loop(0, nx, body, 0)

    def x_pass(s):
        buf = bufs[s]
        eps = eps_of(CELL_SIZE)

        def body(first, i, carry):
            k = first + i // tiles
            base = pl.multiple_of(lax.rem(i, tiles) * 8, 8)
            rows, rows_acc = pl.ds(base + PAD, 8), pl.ds(base, 8)
            row = flow_row(0, k)
            dt = step[...]
            u = [buf[j, 3 + k, rows, :] for j in range(nx + 6)]
            q = [u[j + 1] - u[j] for j in range(nx + 5)]
            d = [q[j + 1] - q[j] for j in range(nx + 4)]
            for x in range(nx):
                fh = (row + wind[0, x, rows_acc, :]) * (1.0 / CELL_SIZE)
                total = acc[x, k, rows_acc, :] + upwind(*d[x:x + 5], q[x + 2], q[x + 3], fh, eps)
                moved = u[x + 3] - dt * jnp.maximum(total, 0.0)
                if s == 0:
                    b1[3 + x, 3 + k, rows, :] = moved
                elif s == 1:
                    b2[3 + x, 3 + k, rows, :] = 0.75 * b0[3 + x, 3 + k, rows, :] + 0.25 * moved
                else:
                    out_ref[x, k, rows_acc, :] = (moved - b0[3 + x, 3 + k, rows, :]) * (2.0 / (3.0 * SCALE))
            return carry

        for c in range(parts):
            mine = (4 + 2 * c, 5 + 2 * c)
            wait_in(s, mine)
            lax.fori_loop(0, part * tiles, functools.partial(body, c * part), 0)
            if s < 2:
                send(s + 1, mine)
        if s < 2:
            send(s + 1, range(4))

    def fill_x(buf):
        def ends(low):
            def act():
                def body(k, carry):
                    edge = buf[3 if low else nx + 2, 3 + k, PAD:PAD + ny, :]
                    slope = edge - buf[4 if low else nx + 1, 3 + k, PAD:PAD + ny, :]
                    for r in range(1, 4):
                        buf[3 - r if low else nx + 2 + r, 3 + k, PAD:PAD + ny, :] = edge + r * slope
                    return carry
                lax.fori_loop(0, nh, body, 0)
            return act
        pl.when(gx == 0)(ends(True))
        pl.when(gx == ngx - 1)(ends(False))

    def fill_y(buf):
        index = lax.broadcasted_iota(jnp.int32, (8, nv), 0).astype(jnp.float32)

        def ends(low):
            reach = (8.0 - index) if low else (index + 1.0)
            at, near, to = (PAD, PAD + 1, 0) if low else (PAD + ny - 1, PAD + ny - 2, PAD + ny)

            def act():
                def body(x, carry):
                    for k in range(nh):
                        edge = buf[3 + x, 3 + k, at:at + 1, :]
                        slope = edge - buf[3 + x, 3 + k, near:near + 1, :]
                        buf[3 + x, 3 + k, to:to + 8, :] = edge + reach * slope
                    return carry
                lax.fori_loop(0, nx, body, 0)
            return act
        pl.when(gy == 0)(ends(True))
        pl.when(gy == ngy - 1)(ends(False))

    for s in range(3):
        if s == 0:
            send(0, range(4 + 2 * parts))
            for copy in rate_copies:
                copy.start()
        v_shift(bufs[s])
        v_pass(bufs[s])
        fill_y(bufs[s])
        fill_x(bufs[s])
        wait_in(s, (2, 3))
        y_pass(bufs[s])
        wait_in(s, (0, 1))
        h_pass(bufs[s])
        if s == 0:
            for copy in rate_copies:
                copy.wait_recv()
            top = best[...]
            for delta in range(1, n_xy):
                top = jnp.maximum(top, peers[delta - 1])
            rate = jnp.max(top, axis=(0, 1), keepdims=True) + (TURN_MAX / d_theta + ACCEL_MAX / d_speed)
            step[...] = jnp.broadcast_to(CFL_NUMBER / rate, step.shape)
        x_pass(s)

    for copy in rate_copies:
        copy.wait_send()
    for s in range(3):
        for copy, has_out, _ in plans[s]:
            under(has_out, copy.wait_send)


def tables(nv, n_head):
    speeds = (SPEED_LOW + SPEED_SPAN * (np.arange(nv, dtype=np.float32) + np.float32(0.5)) / nv).astype(np.float32)
    angles = np.arange(n_head, dtype=np.float32) * np.float32(2.0 * math.pi / n_head)
    turns = np.stack([np.cos(angles.astype(np.float64)), np.sin(angles.astype(np.float64))]).astype(np.float32)
    flow = turns[:, :, None] * speeds[None, None, :]
    ends = np.concatenate([flow[:, :, 0], flow[:, :, -1]], axis=1)
    rows = -(-ends.shape[1] // 128)
    ends = np.concatenate([ends, np.repeat(ends[:, :1], rows * 128 - ends.shape[1], axis=1)], axis=1)
    return flow, ends.reshape(2, rows, 128)


def solution(mesh):
    axes = (mesh.shape["gx"], mesh.shape["gy"], mesh.shape["ha"])

    def body(level_set, wind_field):
        nx, ny, nh, nv = level_set.shape
        flow, ends = tables(nv, nh * axes[2])
        n_xy = axes[0] * axes[1]
        state = pltpu.VMEM((nx + 6, nh + 6, ny + 2 * PAD, nv), jnp.float32)
        vmem = pl.BlockSpec(memory_space=pltpu.VMEM)
        increment = pl.pallas_call(
            functools.partial(kernel, (nx, ny, nh, nv), axes),
            out_shape=jax.ShapeDtypeStruct((nx, nh, ny, nv), jnp.float32),
            in_specs=[vmem, pl.BlockSpec(memory_space=pltpu.SMEM), vmem, vmem],
            out_specs=vmem,
            scratch_shapes=[
                state, state, state,
                pltpu.VMEM((nx, nh, ny, nv), jnp.float32),
                pltpu.VMEM((5, nx, nh, ny, nv), jnp.float32),
                pltpu.VMEM((nx, nh, ny, nv), jnp.float32),
                pltpu.VMEM((2, nx, ny, nv), jnp.float32),
                pltpu.VMEM((8, 128), jnp.float32),
                pltpu.VMEM((n_xy - 1, 8, 128), jnp.float32),
                pltpu.VMEM((8, nv), jnp.float32),
                pltpu.SemaphoreType.DMA((3, 4 + 2 * math.gcd(nh, 5))),
                pltpu.SemaphoreType.DMA((3, 4 + 2 * math.gcd(nh, 5))),
                pltpu.SemaphoreType.DMA((n_xy - 1,)),
                pltpu.SemaphoreType.DMA((n_xy - 1,)),
            ],
            compiler_params=pltpu.CompilerParams(
                collective_id=0, has_side_effects=True, vmem_limit_bytes=56 * 2**20
            ),
        )(level_set.transpose(0, 2, 1, 3), wind_field, jnp.asarray(flow), jnp.asarray(ends))
        return increment.transpose(0, 2, 1, 3)

    return jax.shard_map(
        body,
        mesh=mesh,
        in_specs=(P("gx", "gy", "ha", None), P(None, "gx", "gy")),
        out_specs=P("gx", "gy", "ha", None),
        check_vma=False,
    )
```
